512 devices in a mesh: ta: 4 (over x), xy: 16 (over z), gz: 8 (over y, core).
Axes of the slice: x: 4, y: 4, z: 16, core: 2. Of those that a mesh axis runs over, the one named last changes fastest.
Arguments:
- propagator: float32 [2, 4, 4, 9, 128, 16384], P(None, None, None, None, 'ta', ('xy', 'gz')), as said below
- site_coords: int32 [3, 16384], P(None, ('xy', 'gz')), may hold values from 0 to 95
- momenta: int32 [3, 64], replicated, may hold values from 1 to 4
- source_slice: int32 [4], replicated, may hold values from 0 to 127
Outputs:
- correlator: float32 [16, 128, 128], P(None, 'ta')
The draws below stay inside these ranges and needn't reach their ends.
Inputs may be any that keep to these rules, and one draw needn't show every extreme that they name: `momenta`: each component of a momentum lies in 1 to 4. `site_coords`: each site coordinate. `propagator`: real-valued entries of order one, with a scale that differs between time slices.
All inputs are finite; a program needn't handle non-finite values.
Results may differ from the reference program's by a relative error of at most 0.000071.
Values sent between devices are 32-bit elements; how exact they have to be, the bound alone decides.
No kernel may reach another device: no remote copies, remote signals or barrier semaphores. Data moves between devices by JAX's collectives and lax.ppermute only.
A program may use at most 64 MiB of HBM per device.

```python
import math
import jax
import jax.numpy as jnp
from jax import lax

SPINS = 4
COLOR_PAIRS = 9
NP = 64
EXTENT = 96
NSRC = 4
NT = 128
SITES = 16384


def draw_propagator(key, part):
    base_key, scale_key = jax.random.split(jax.random.fold_in(key, 11))
    shape = (2, SPINS, SPINS, COLOR_PAIRS, NT, SITES)
    scales = jnp.exp(jax.random.uniform(scale_key, (NT,), jnp.float32, -0.7, 0.7))
    values = jax.random.normal(base_key, shape, jnp.float32)
    return (values * scales[:, None]).astype(jnp.float32)


def touch_ends(result, rng, low, top_value):
    index_at = [jax.random.randint(jax.random.fold_in(rng, axis), (), 0, length) for axis, length in enumerate(result.shape)]
    main_axis = result.shape.index(max(result.shape))
    beside = index_at[:main_axis] + [(index_at[main_axis] + 1) % result.shape[main_axis]] + index_at[main_axis + 1:]
    return result.at[tuple(index_at)].set(low).at[tuple(beside)].set(top_value)


def setup_inputs(seed: int = 0) -> dict:
    key_list = jax.random.split(jax.random.key(seed), 5)
    propagator = draw_propagator(jax.random.fold_in(key_list[4], 71), 0)
    site_coords = touch_ends(jax.random.randint(key_list[1], (3, SITES), 0, EXTENT), jax.random.fold_in(key_list[1], 1), 0, EXTENT - 1).astype(jnp.int32)
    momenta = touch_ends(jax.random.randint(key_list[2], (3, NP), 1, 5), jax.random.fold_in(key_list[2], 1), 1, 4).astype(jnp.int32)
    source_slice = touch_ends(jax.random.randint(key_list[3], (NSRC,), 0, NT), jax.random.fold_in(key_list[3], 1), 0, NT - 1).astype(jnp.int32)
    return {"propagator": propagator, "site_coords": site_coords, "momenta": momenta, "source_slice": source_slice}


def phase_table(site_coords, momenta):
    turns = jnp.dot(site_coords.T.astype(jnp.int32), momenta.astype(jnp.int32))
    turns = jnp.remainder(turns, EXTENT).astype(jnp.int32)
    angles = turns.astype(jnp.float32) * jnp.float32(2.0 * math.pi / EXTENT)
    return jnp.concatenate([jnp.cos(angles), -jnp.sin(angles)], axis=1)

def reference(propagator, site_coords, momenta, source_slice):
    phases = phase_table(site_coords, momenta)

    def one_slice(index):
        block = lax.dynamic_slice_in_dim(propagator, index, 1, 4)
        density = lax.optimization_barrier(jnp.sum(jnp.square(block), axis=(0, 3))).reshape(SPINS * SPINS, SITES)
        projected = jnp.dot(density, phases, precision=lax.Precision.HIGHEST, preferred_element_type=jnp.float32)
        return (projected, jnp.sum(density))
    projected, slice_total = lax.map(one_slice, jnp.arange(NT, dtype=jnp.int32))
    projected = jnp.transpose(projected, (1, 0, 2))
    picked = jnp.arange(NT, dtype=jnp.int32)[:, None] == source_slice.astype(jnp.int32)[None, :]
    counts = lax.optimization_barrier(jnp.sum(picked.astype(jnp.float32), axis=1))
    grand_total = jnp.maximum(jnp.sum(counts * slice_total), jnp.float32(SITES))
    slice_norm = jnp.maximum(slice_total, jnp.float32(SITES))
    return projected * jnp.sqrt(grand_total) / slice_norm[None, :, None]
```

```python
import math

import jax
import jax.numpy as jnp
from jax import lax
from jax.sharding import Mesh
from jax.sharding import PartitionSpec as P

EXTENT = 96
GZ = ("gz_0", "gz_1")
NEAR = ("z_lo", "gz_0", "gz_1")
FAR = "z_hi"
SITE_AXES = ("z_hi", "z_lo", "gz_0", "gz_1")


def exchange(x, axes):
    return lax.all_to_all(x, axes, split_axis=0, concat_axis=0, tiled=True)


def copies(x, axes):
    return jnp.broadcast_to(x, (lax.axis_size(axes), *x.shape))


def phase_table(site_coords, momenta):
    turns = jnp.dot(site_coords.T, momenta)
    turns = jnp.remainder(turns, EXTENT)
    angles = turns.astype(jnp.float32) * jnp.float32(2.0 * math.pi / EXTENT)
    return jnp.concatenate([jnp.cos(angles), -jnp.sin(angles)], axis=1)


def on_device(propagator, site_coords, momenta, source_slice):
    slices = propagator.shape[4]
    local_sites = propagator.shape[5]
    pairs = propagator.shape[1] * propagator.shape[2]
    near = lax.axis_size(NEAR)
    rows = pairs * slices // near
    phases = phase_table(site_coords, momenta)
    density = jnp.sum(jnp.square(propagator), axis=(0, 3)).reshape(pairs * slices, local_sites)
    partial_value = jnp.dot(
        density, phases, precision=lax.Precision.HIGHEST, preferred_element_type=jnp.float32
    )
    lanes = partial_value.shape[1]
    slice_total = jnp.sum(density.reshape(pairs, slices, local_sites), axis=(0, 2))
    stats = jnp.pad(slice_total, (0, lanes - slices))

    blocks = partial_value.reshape(near, rows, 1, lanes)
    blocks = jnp.concatenate([blocks, copies(stats[None, None, :], NEAR)], axis=1)
    near_sum = jnp.sum(exchange(blocks, NEAR), axis=0)
    far_sum = jnp.sum(exchange(copies(near_sum, FAR), FAR), axis=0)

    plane_total = far_sum[rows, 0, :slices]
    offset = lax.axis_index("ta") * slices
    picked = jnp.arange(slices, dtype=jnp.int32)[:, None] + offset == source_slice[None, :]
    counts = jnp.sum(picked.astype(jnp.float32), axis=1)
    mine = jnp.broadcast_to(jnp.sum(counts * plane_total), (1, lanes))
    grand_total = jnp.sum(exchange(copies(mine, "ta"), "ta")[:, 0, 0])

    all_sites = jnp.float32(local_sites * lax.axis_size(SITE_AXES))
    scaled = far_sum[:rows, 0, :].reshape(rows // slices, slices, lanes)
    scaled = scaled / jnp.maximum(plane_total, all_sites)[None, :, None]
    gathered = exchange(copies(scaled.reshape(rows, lanes), NEAR), NEAR)
    correlator = gathered * jnp.sqrt(jnp.maximum(grand_total, all_sites))
    return correlator.reshape(pairs, slices, lanes)


def solution(mesh):
    finer = Mesh(
        mesh.devices.reshape(mesh.shape["ta"], mesh.shape["xy"] // 2, 2, 4, 2),
        ("ta", "z_hi", "z_lo", "gz_0", "gz_1"),
    )
    return jax.shard_map(
        on_device,
        mesh=finer,
        in_specs=(P(None, None, None, None, "ta", SITE_AXES), P(None, SITE_AXES), P(), P()),
        out_specs=P(None, "ta", None),
        check_vma=False,
    )
```

```python
import functools
import math

import jax
import jax.numpy as jnp
from jax import lax
from jax.experimental import pallas as pl
from jax.experimental.pallas import tpu as pltpu
from jax.sharding import PartitionSpec as P

EXTENT = 96
SITE_AXES = ("xy", "gz")
IN_HBM = pl.BlockSpec(memory_space=pltpu.HBM)
IN_VMEM = pl.BlockSpec(memory_space=pltpu.VMEM)


def plane(pair, member, pairs):
    return 2 * pair + (member if 2 * pair < pairs else 1 - member)


def groups(planes, blocks):
    pairs = planes // 2
    near = [
        [plane(p, m, pairs) * blocks + g for m in range(2) for g in range(blocks)]
        for p in range(pairs)
    ]
    far = [[plane(p, m, pairs) for p in range(pairs)] for m in range(2)]
    return near, far


def exchange(x, axes, axis_groups=None):
    return lax.all_to_all(
        x, axes, split_axis=0, concat_axis=0, tiled=True, axis_index_groups=axis_groups
    )


def phase_table(coords, momenta):
    both = jnp.concatenate([momenta, momenta], axis=1)
    turns = lax.dot_general(
        coords, both, (((0,), (0,)), ((), ())), preferred_element_type=jnp.float32
    )
    lane = lax.broadcasted_iota(jnp.int32, turns.shape, 1)
    turns = turns + jnp.where(lane >= momenta.shape[1], EXTENT / 4.0, 0.0)
    turns = turns - EXTENT * jnp.floor((turns + 0.5) * (1.0 / EXTENT))
    angle = (jnp.abs(turns - EXTENT / 2.0) - EXTENT / 4.0) * (2.0 * math.pi / EXTENT)
    square = angle * angle
    series = jnp.full_like(square, 1.0 / math.factorial(13))
    for power in (11, 9, 7, 5, 3, 1):
        sign = -1.0 if power % 4 == 3 else 1.0
        series = series * square + sign / math.factorial(power)
    return series * angle


def project_kernel(
    near, propagator, coords, momenta, source, out, parts, site_buf, mom_buf, src_buf, density,
    total, part_sem, small_sem,
):
    _, sinks, sources, colors, slices, _ = propagator.shape
    pairs = sinks * sources
    lanes = out.shape[1]
    rows = pairs * slices // near
    loads = [
        pltpu.make_async_copy(coords, site_buf, small_sem.at[0]),
        pltpu.make_async_copy(momenta, mom_buf, small_sem.at[1]),
        pltpu.make_async_copy(source, src_buf, small_sem.at[2]),
    ]
    for load in loads:
        load.start()
    copies = [
        pltpu.make_async_copy(
            propagator.at[:, p // sources, p % sources], parts.at[p], part_sem.at[p]
        )
        for p in range(pairs)
    ]
    for copy in copies:
        copy.start()
    for load in loads:
        load.wait()
    phases = phase_table(site_buf[...].astype(jnp.float32), mom_buf[...].astype(jnp.float32))
    first = lax.axis_index("ta") * slices
    lane = lax.broadcasted_iota(jnp.int32, (8, lanes), 1)
    counts = jnp.zeros((8, lanes), jnp.float32)
    for i in range(source.shape[0]):
        counts = counts + jnp.where(lane == src_buf[i] - first, 1.0, 0.0)
    total[...] = jnp.zeros_like(total)
    step = 4
    over_pairs = None
    for p in range(pairs):
        copies[p].wait()
        value = None
        for r in range(2):
            for c in range(colors):
                part = parts[p, r, c]
                value = part * part if value is None else value + part * part
        density[p * slices : (p + 1) * slices] = value
        over_pairs = value if over_pairs is None else over_pairs + value
        if p % step == step - 1:
            begin = (p + 1 - step) * slices
            projected = jnp.dot(
                density[begin : begin + step * slices],
                phases,
                precision=lax.Precision.HIGHEST,
                preferred_element_type=jnp.float32,
            )
            for part in range(step * slices // rows):
                block = begin // rows + part
                out[block * (rows + 1) : block * (rows + 1) + rows] = projected[
                    part * rows : (part + 1) * rows
                ]
    total[:slices] = over_pairs
    by_slice = lax.dot_general(
        jnp.ones((8, total.shape[1]), jnp.float32),
        total[...],
        (((1,), (1,)), ((), ())),
        precision=lax.Precision.HIGHEST,
        preferred_element_type=jnp.float32,
    )
    picked = jnp.sum(by_slice * counts, axis=1, keepdims=True)
    stats = jnp.where(lane < slices, by_slice, picked)
    for block in range(near):
        out[block * (rows + 1) + rows : (block + 1) * (rows + 1)] = stats[:1]


def project(propagator, coords, momenta, source, near):
    _, sinks, sources, colors, slices, sites = propagator.shape
    pairs = sinks * sources
    lanes = 2 * momenta.shape[1]
    return pl.pallas_call(
        functools.partial(project_kernel, near),
        out_shape=jax.ShapeDtypeStruct((pairs * slices + near, lanes), jnp.float32),
        in_specs=[IN_HBM] * 4,
        out_specs=IN_VMEM,
        scratch_shapes=[
            pltpu.VMEM((pairs, 2, colors, slices, sites), jnp.float32),
            pltpu.VMEM(coords.shape, jnp.int32),
            pltpu.VMEM(momenta.shape, jnp.int32),
            pltpu.SMEM(source.shape, jnp.int32),
            pltpu.VMEM((pairs * slices, sites), jnp.float32),
            pltpu.VMEM((lanes, sites), jnp.float32),
            pltpu.SemaphoreType.DMA((pairs,)),
            pltpu.SemaphoreType.DMA((3,)),
        ],
        compiler_params=pltpu.CompilerParams(vmem_limit_bytes=12 << 20),
    )(*[pltpu.with_memory_space_constraint(x, pltpu.HBM) for x in (propagator, coords, momenta, source)])


def sum_of_blocks(ref, blocks):
    rows = ref.shape[0] // blocks
    value = ref[:rows]
    for b in range(1, blocks):
        value = value + ref[b * rows : (b + 1) * rows]
    return value


def near_kernel(near, far, received, out):
    value = sum_of_blocks(received, near)
    rows = value.shape[0]
    for b in range(far):
        out[b * rows : (b + 1) * rows] = value


def far_kernel(far, slices, floor, received, out, picked):
    value = sum_of_blocks(received, far)
    rows = value.shape[0] - 1
    lanes = value.shape[1]
    stats = value[rows:]
    row = lax.broadcasted_iota(jnp.int32, (slices, lanes), 0)
    lane = lax.broadcasted_iota(jnp.int32, (slices, lanes), 1)
    column = jnp.sum(jnp.where(row == lane, stats, 0.0), axis=1, keepdims=True)
    norm = jnp.maximum(column, floor)
    for pair in range(rows // slices):
        scaled = value[pair * slices : (pair + 1) * slices] / norm
        for b in range(out.shape[0]):
            out[b, pair * slices : (pair + 1) * slices] = scaled
    picked[...] = stats


def scale_kernel(floor, gathered, *refs):
    *picked, out, buf, sems = refs
    total = picked[0][...]
    for other in picked[1:]:
        total = total + other[...]
    factor = jnp.sqrt(jnp.maximum(total, floor))[:, out.shape[2] - 1 :]
    pieces = sems.shape[0]
    size = gathered.shape[0] // pieces
    copies = []
    for i in range(pieces):
        part = slice(i * size, (i + 1) * size)
        buf[part] = gathered[part] * factor[None]
        copies.append(pltpu.make_async_copy(buf.at[part], out.at[part], sems.at[i]))
        copies[-1].start()
    for copy in copies:
        copy.wait()


SMALL = pltpu.CompilerParams(vmem_limit_bytes=4 << 20)


def on_device(near_groups, far_groups, propagator, site_coords, momenta, source_slice):
    _, sinks, sources, _, slices, local_sites = propagator.shape
    pairs = sinks * sources
    lanes = 2 * momenta.shape[1]
    near = len(near_groups[0])
    far = len(far_groups[0])
    times = lax.axis_size("ta")
    rows = pairs * slices // near
    all_sites = float(local_sites * lax.axis_size(SITE_AXES))
    blocks = project(propagator, site_coords, momenta, source_slice, near)
    received = exchange(blocks.reshape(near, rows + 1, 1, lanes), SITE_AXES, near_groups)
    blocks = pl.pallas_call(
        functools.partial(near_kernel, near, far),
        out_shape=jax.ShapeDtypeStruct((far * (rows + 1), lanes), jnp.float32),
        in_specs=[IN_VMEM],
        out_specs=IN_VMEM,
        compiler_params=SMALL,
    )(received.reshape(near * (rows + 1), lanes))
    received = exchange(blocks.reshape(far, rows + 1, 1, lanes), "xy", far_groups)
    scaled, picked = pl.pallas_call(
        functools.partial(far_kernel, far, slices, all_sites),
        out_shape=(
            jax.ShapeDtypeStruct((near, rows, lanes), jnp.float32),
            jax.ShapeDtypeStruct((1, lanes), jnp.float32),
        ),
        in_specs=[IN_VMEM],
        out_specs=(IN_VMEM, IN_VMEM),
        compiler_params=SMALL,
    )(received.reshape(far * (rows + 1), lanes))
    gathered = exchange(scaled, SITE_AXES, near_groups)
    totals = [picked]
    for k in range(1, times):
        swap = [(t, t ^ k) for t in range(times)]
        totals.append(lax.ppermute(picked, "ta", swap))
    correlator = pl.pallas_call(
        functools.partial(scale_kernel, all_sites),
        out_shape=jax.ShapeDtypeStruct((pairs, slices, lanes), jnp.float32),
        in_specs=[IN_VMEM] * (1 + times),
        out_specs=pl.BlockSpec(memory_space=pltpu.HBM),
        scratch_shapes=[
            pltpu.VMEM((pairs, slices, lanes), jnp.float32),
            pltpu.SemaphoreType.DMA((4,)),
        ],
        compiler_params=SMALL,
    )(gathered.reshape(pairs, slices, lanes), *totals)
    return correlator


def solution(mesh):
    near_groups, far_groups = groups(mesh.shape["xy"], mesh.shape["gz"])
    return jax.shard_map(
        functools.partial(on_device, near_groups, far_groups),
        mesh=mesh,
        in_specs=(P(None, None, None, None, "ta", SITE_AXES), P(None, SITE_AXES), P(), P()),
        out_specs=P(None, "ta", None),
        check_vma=False,
    )
```

```python
import functools
import math

import jax
import jax.numpy as jnp
from jax import lax
from jax.experimental import pallas as pl
from jax.experimental.pallas import tpu as pltpu
from jax.sharding import PartitionSpec as P

EXTENT = 96
SITE_AXES = ("xy", "gz")
IN_HBM = pl.BlockSpec(memory_space=pltpu.HBM)
IN_VMEM = pl.BlockSpec(memory_space=pltpu.VMEM)


def groups(planes, blocks):
    pairs = planes // 2
    swapped = range(pairs // 4, pairs - pairs // 4)
    plane = [[2 * p + (m ^ (p in swapped)) for m in range(2)] for p in range(pairs)]
    alternate = [b for start in (0, blocks // 2) for b in range(start, start + blocks // 2)]
    alternate = [alternate[(i % 2) * (blocks // 2) + i // 2] for i in range(blocks)]
    cores = [b for core in range(2) for b in alternate if b % 2 == core]
    near = [[plane[p][m] * blocks + b for b in cores for m in range(2)] for p in range(pairs)]
    half = pairs // 2
    far = [[plane[(i % 2) * half + i // 2][m] for i in range(pairs)] for m in range(2)]
    return near, far


def exchange(x, axes, axis_groups=None):
    return lax.all_to_all(
        x, axes, split_axis=0, concat_axis=0, tiled=True, axis_index_groups=axis_groups
    )


def phase_table(coords, momenta):
    both = jnp.concatenate([momenta, momenta], axis=1)
    turns = lax.dot_general(
        coords, both, (((0,), (0,)), ((), ())), preferred_element_type=jnp.float32
    )
    lane = lax.broadcasted_iota(jnp.int32, turns.shape, 1)
    turns = turns + jnp.where(lane >= momenta.shape[1], EXTENT / 4.0, 0.0)
    turns = turns - EXTENT * jnp.floor((turns + 0.5) * (1.0 / EXTENT))
    angle = (jnp.abs(turns - EXTENT / 2.0) - EXTENT / 4.0) * (2.0 * math.pi / EXTENT)
    square = angle * angle
    series = jnp.full_like(square, 1.0 / math.factorial(13))
    for power in (11, 9, 7, 5, 3, 1):
        sign = -1.0 if power % 4 == 3 else 1.0
        series = series * square + sign / math.factorial(power)
    return series * angle


def project_kernel(
    near, propagator, coords, momenta, source, out, parts, site_buf, mom_buf, src_buf, density,
    part_sem, small_sem,
):
    _, sinks, sources, colors, slices, _ = propagator.shape
    pairs = sinks * sources
    step = pairs // part_sem.shape[0]
    lanes = out.shape[1]
    rows = pairs * slices // near
    loads = [
        pltpu.make_async_copy(coords, site_buf, small_sem.at[0]),
        pltpu.make_async_copy(momenta, mom_buf, small_sem.at[1]),
        pltpu.make_async_copy(source, src_buf, small_sem.at[2]),
    ]
    for load in loads:
        load.start()
    copies = [
        pltpu.make_async_copy(
            propagator.at[:, p // sources, pl.ds(p % sources, step)],
            parts.at[:, pl.ds(p, step)],
            part_sem.at[p // step],
        )
        for p in range(0, pairs, step)
    ]
    for copy in copies:
        copy.start()
    for load in loads:
        load.wait()
    phases = phase_table(site_buf[...].astype(jnp.float32), mom_buf[...].astype(jnp.float32))
    first = lax.axis_index("ta") * slices
    row = lax.broadcasted_iota(jnp.int32, (slices, lanes), 0)
    lane = lax.broadcasted_iota(jnp.int32, (slices, lanes), 1)
    weight = jnp.zeros((slices, lanes), jnp.float32)
    for i in range(source.shape[0]):
        weight = weight + jnp.where(row == src_buf[i] - first, 1.0, 0.0)
    weight = jnp.where(lane < slices, jnp.where(row == lane, 1.0, 0.0), weight)
    over_pairs = None
    for p in range(pairs):
        if p % step == 0:
            copies[p // step].wait()
        value = None
        for r in range(2):
            for c in range(colors):
                part = parts[r, p, c]
                value = part * part if value is None else value + part * part
        density[p * slices : (p + 1) * slices] = value
        over_pairs = value if over_pairs is None else over_pairs + value
    by_slice = jnp.sum(over_pairs, axis=1, keepdims=True)
    stats = jnp.sum(by_slice * weight, axis=0, keepdims=True)
    projected = jnp.dot(
        density[...],
        phases,
        precision=lax.Precision.HIGHEST,
        preferred_element_type=jnp.float32,
    )
    for block in range(near):
        begin = block * (rows + 1)
        out[begin : begin + rows] = projected[block * rows : (block + 1) * rows]
        out[begin + rows : begin + rows + 1] = stats


def project(propagator, coords, momenta, source, near):
    _, sinks, sources, colors, slices, sites = propagator.shape
    pairs = sinks * sources
    lanes = 2 * momenta.shape[1]
    arrays = (propagator, coords, momenta, source)
    return pl.pallas_call(
        functools.partial(project_kernel, near),
        out_shape=jax.ShapeDtypeStruct((pairs * slices + near, lanes), jnp.float32),
        in_specs=[IN_HBM] * 4,
        out_specs=IN_VMEM,
        scratch_shapes=[
            pltpu.VMEM((2, pairs, colors, slices, sites), jnp.float32),
            pltpu.VMEM(coords.shape, jnp.int32),
            pltpu.VMEM(momenta.shape, jnp.int32),
            pltpu.SMEM(source.shape, jnp.int32),
            pltpu.VMEM((pairs * slices, sites), jnp.float32),
            pltpu.SemaphoreType.DMA((pairs // 2,)),
            pltpu.SemaphoreType.DMA((3,)),
        ],
        compiler_params=pltpu.CompilerParams(vmem_limit_bytes=12 << 20),
    )(*[pltpu.with_memory_space_constraint(x, pltpu.HBM) for x in arrays])


def sum_of_blocks(ref, blocks):
    rows = ref.shape[0] // blocks
    value = ref[:rows]
    for b in range(1, blocks):
        value = value + ref[b * rows : (b + 1) * rows]
    return value


def near_kernel(near, far, received, out):
    value = sum_of_blocks(received, near)
    rows = value.shape[0]
    for b in range(far):
        out[b * rows : (b + 1) * rows] = value


def far_kernel(far, slices, floor, received, out, picked):
    value = sum_of_blocks(received, far)
    rows = value.shape[0] - 1
    lanes = value.shape[1]
    stats = value[rows:]
    row = lax.broadcasted_iota(jnp.int32, (slices, lanes), 0)
    lane = lax.broadcasted_iota(jnp.int32, (slices, lanes), 1)
    column = jnp.sum(jnp.where(row == lane, stats, 0.0), axis=1, keepdims=True)
    norm = jnp.maximum(column, floor)
    for pair in range(rows // slices):
        scaled = value[pair * slices : (pair + 1) * slices] / norm
        for b in range(out.shape[0]):
            out[b, pair * slices : (pair + 1) * slices] = scaled
    picked[...] = stats


def scale_kernel(floor, gathered, total, out, buf, sems):
    factor = jnp.sqrt(jnp.maximum(total[...], floor))[:, out.shape[2] - 1 :]
    pieces = sems.shape[0]
    size = gathered.shape[0] // pieces
    copies = []
    for i in range(pieces):
        part = slice(i * size, (i + 1) * size)
        buf[part] = gathered[part] * factor[None]
        copies.append(pltpu.make_async_copy(buf.at[part], out.at[part], sems.at[i]))
        copies[-1].start()
    for copy in copies:
        copy.wait()


SMALL = pltpu.CompilerParams(vmem_limit_bytes=4 << 20)


def on_device(near_groups, far_groups, propagator, site_coords, momenta, source_slice):
    _, sinks, sources, _, slices, local_sites = propagator.shape
    pairs = sinks * sources
    lanes = 2 * momenta.shape[1]
    near = len(near_groups[0])
    far = len(far_groups[0])
    rows = pairs * slices // near
    all_sites = float(local_sites * lax.axis_size(SITE_AXES))
    blocks = project(propagator, site_coords, momenta, source_slice, near)
    received = exchange(blocks.reshape(near, rows + 1, 1, lanes), SITE_AXES, near_groups)
    blocks = pl.pallas_call(
        functools.partial(near_kernel, near, far),
        out_shape=jax.ShapeDtypeStruct((far * (rows + 1), lanes), jnp.float32),
        in_specs=[IN_VMEM],
        out_specs=IN_VMEM,
        compiler_params=SMALL,
    )(received.reshape(near * (rows + 1), lanes))
    received = exchange(blocks.reshape(far, rows + 1, 1, lanes), "xy", far_groups)
    scaled, picked = pl.pallas_call(
        functools.partial(far_kernel, far, slices, all_sites),
        out_shape=(
            jax.ShapeDtypeStruct((near, rows, lanes), jnp.float32),
            jax.ShapeDtypeStruct((1, lanes), jnp.float32),
        ),
        in_specs=[IN_VMEM],
        out_specs=(IN_VMEM, IN_VMEM),
        compiler_params=SMALL,
    )(received.reshape(far * (rows + 1), lanes))
    gathered = exchange(scaled, SITE_AXES, near_groups)
    picked = lax.psum(picked, "ta")
    correlator = pl.pallas_call(
        functools.partial(scale_kernel, all_sites),
        out_shape=jax.ShapeDtypeStruct((pairs, slices, lanes), jnp.float32),
        in_specs=[IN_VMEM] * 2,
        out_specs=pl.BlockSpec(memory_space=pltpu.HBM),
        scratch_shapes=[
            pltpu.VMEM((pairs, slices, lanes), jnp.float32),
            pltpu.SemaphoreType.DMA((2,)),
        ],
        compiler_params=SMALL,
    )(gathered.reshape(pairs, slices, lanes), picked)
    return correlator


def solution(mesh):
    near_groups, far_groups = groups(mesh.shape["xy"], mesh.shape["gz"])
    return jax.shard_map(
        functools.partial(on_device, near_groups, far_groups),
        mesh=mesh,
        in_specs=(P(None, None, None, None, "ta", SITE_AXES), P(None, SITE_AXES), P(), P()),
        out_specs=P(None, "ta", None),
        check_vma=False,
    )
```

```python
import functools
import math

import jax
import jax.numpy as jnp
from jax import lax
from jax.experimental import pallas as pl
from jax.experimental.pallas import tpu as pltpu
from jax.sharding import PartitionSpec as P

EXTENT = 96
SITE_AXES = ("xy", "gz")
IN_HBM = pl.BlockSpec(memory_space=pltpu.HBM)
IN_VMEM = pl.BlockSpec(memory_space=pltpu.VMEM)


def groups(planes, blocks):
    pairs = planes // 2
    swapped = range(pairs // 4, pairs - pairs // 4)
    plane = [[2 * p + (m ^ (p in swapped)) for m in range(2)] for p in range(pairs)]
    alternate = [b for start in (0, blocks // 2) for b in range(start, start + blocks // 2)]
    alternate = [alternate[(i % 2) * (blocks // 2) + i // 2] for i in range(blocks)]
    cores = [b for core in range(2) for b in alternate if b % 2 == core]
    near = [[plane[p][m] * blocks + b for b in cores for m in range(2)] for p in range(pairs)]
    half = pairs // 2
    far = [[plane[(i % 2) * half + i // 2][m] for i in range(pairs)] for m in range(2)]
    return near, far


def exchange(x, axes, axis_groups=None):
    return lax.all_to_all(
        x, axes, split_axis=0, concat_axis=0, tiled=True, axis_index_groups=axis_groups
    )


def phase_table(coords, momenta):
    both = jnp.concatenate([momenta, momenta], axis=1)
    turns = lax.dot_general(
        coords, both, (((0,), (0,)), ((), ())), preferred_element_type=jnp.float32
    )
    lane = lax.broadcasted_iota(jnp.int32, turns.shape, 1)
    turns = turns + jnp.where(lane >= momenta.shape[1], EXTENT / 4.0, 0.0)
    turns = turns - EXTENT * jnp.floor((turns + 0.5) * (1.0 / EXTENT))
    angle = (jnp.abs(turns - EXTENT / 2.0) - EXTENT / 4.0) * (2.0 * math.pi / EXTENT)
    square = angle * angle
    series = jnp.full_like(square, 1.0 / math.factorial(13))
    for power in (11, 9, 7, 5, 3, 1):
        sign = -1.0 if power % 4 == 3 else 1.0
        series = series * square + sign / math.factorial(power)
    return series * angle


def project_kernel(
    near, propagator, coords, momenta, source, out, mine, parts, site_buf, mom_buf, src_buf,
    density, blocks, part_sem, small_sem, out_sem,
):
    _, sinks, sources, colors, slices, _ = propagator.shape
    pairs = sinks * sources
    step = pairs // part_sem.shape[0]
    lanes = out.shape[1]
    rows = pairs * slices // near
    loads = [
        pltpu.make_async_copy(coords, site_buf, small_sem.at[0]),
        pltpu.make_async_copy(momenta, mom_buf, small_sem.at[1]),
        pltpu.make_async_copy(source, src_buf, small_sem.at[2]),
    ]
    for load in loads:
        load.start()
    copies = [
        pltpu.make_async_copy(
            propagator.at[:, p // sources, pl.ds(p % sources, step)],
            parts.at[:, pl.ds(p, step)],
            part_sem.at[p // step],
        )
        for p in range(0, pairs, step)
    ]
    for copy in copies:
        copy.start()
    for load in loads:
        load.wait()
    phases = phase_table(site_buf[...].astype(jnp.float32), mom_buf[...].astype(jnp.float32))
    first = lax.axis_index("ta") * slices
    row = lax.broadcasted_iota(jnp.int32, (slices, lanes), 0)
    lane = lax.broadcasted_iota(jnp.int32, (slices, lanes), 1)
    weight = jnp.zeros((slices, lanes), jnp.float32)
    for i in range(source.shape[0]):
        weight = weight + jnp.where(row == src_buf[i] - first, 1.0, 0.0)
    weight = jnp.where(lane < slices, jnp.where(row == lane, 1.0, 0.0), weight)
    over_pairs = None
    for p in range(pairs):
        if p % step == 0:
            copies[p // step].wait()
        value = None
        for r in range(2):
            for c in range(colors):
                part = parts[r, p, c]
                value = part * part if value is None else value + part * part
        density[p * slices : (p + 1) * slices] = value
        over_pairs = value if over_pairs is None else over_pairs + value
    by_slice = jnp.sum(over_pairs, axis=1, keepdims=True)
    stats = jnp.sum(by_slice * weight, axis=0, keepdims=True)
    mine[...] = stats
    projected = jnp.dot(
        density[...],
        phases,
        precision=lax.Precision.HIGHEST,
        preferred_element_type=jnp.float32,
    )
    stores = []
    size = blocks.shape[0] // out_sem.shape[0]
    for block in range(near):
        begin = block * (rows + 1)
        blocks[begin : begin + rows] = projected[block * rows : (block + 1) * rows]
        blocks[begin + rows : begin + rows + 1] = stats
        if (begin + rows + 1) % size == 0:
            part = pl.ds(size * len(stores), size)
            stores.append(
                pltpu.make_async_copy(blocks.at[part], out.at[part], out_sem.at[len(stores)])
            )
            stores[-1].start()
    for store in stores:
        store.wait()


def project(propagator, coords, momenta, source, near):
    _, sinks, sources, colors, slices, sites = propagator.shape
    pairs = sinks * sources
    lanes = 2 * momenta.shape[1]
    arrays = (propagator, coords, momenta, source)
    return pl.pallas_call(
        functools.partial(project_kernel, near),
        out_shape=(
            jax.ShapeDtypeStruct((pairs * slices + near, lanes), jnp.float32),
            jax.ShapeDtypeStruct((1, lanes), jnp.float32),
        ),
        in_specs=[IN_HBM] * 4,
        out_specs=(IN_HBM, IN_VMEM),
        scratch_shapes=[
            pltpu.VMEM((2, pairs, colors, slices, sites), jnp.float32),
            pltpu.VMEM(coords.shape, jnp.int32),
            pltpu.VMEM(momenta.shape, jnp.int32),
            pltpu.SMEM(source.shape, jnp.int32),
            pltpu.VMEM((pairs * slices, sites), jnp.float32),
            pltpu.VMEM((pairs * slices + near, lanes), jnp.float32),
            pltpu.SemaphoreType.DMA((pairs // 2,)),
            pltpu.SemaphoreType.DMA((3,)),
            pltpu.SemaphoreType.DMA((2,)),
        ],
        compiler_params=pltpu.CompilerParams(vmem_limit_bytes=12 << 20),
    )(*[pltpu.with_memory_space_constraint(x, pltpu.HBM) for x in arrays])


def sum_of_blocks(ref, blocks):
    rows = ref.shape[0] // blocks
    value = ref[:rows]
    for b in range(1, blocks):
        value = value + ref[b * rows : (b + 1) * rows]
    return value


def near_kernel(near, far, slices, received, picked, out):
    value = sum_of_blocks(received, near)
    rows, lanes = value.shape
    lane = lax.broadcasted_iota(jnp.int32, (1, lanes), 1)
    stats = jnp.where(lane < slices, value[rows - 1 :], picked[...])
    for b in range(far):
        out[b * rows : (b + 1) * rows - 1] = value[: rows - 1]
        out[(b + 1) * rows - 1 : (b + 1) * rows] = stats


def far_kernel(near, far, slices, floor, received, out):
    value = sum_of_blocks(received, far)
    rows = value.shape[0] - 1
    lanes = value.shape[1]
    stats = value[rows:]
    row = lax.broadcasted_iota(jnp.int32, (slices, lanes), 0)
    lane = lax.broadcasted_iota(jnp.int32, (slices, lanes), 1)
    column = jnp.sum(jnp.where(row == lane, stats, 0.0), axis=1, keepdims=True)
    norm = jnp.maximum(column, floor)
    for pair in range(rows // slices):
        scaled = value[pair * slices : (pair + 1) * slices] / norm
        for b in range(near):
            begin = b * (rows + 1) + pair * slices
            out[begin : begin + slices] = scaled
    for b in range(near):
        out[b * (rows + 1) + rows : (b + 1) * (rows + 1)] = stats


def scale_kernel(near, floor, gathered, out, buf, sems):
    rows = gathered.shape[0] // near - 1
    total = gathered[rows : rows + 1]
    for b in range(1, near):
        total = total + gathered[b * (rows + 1) + rows : (b + 1) * (rows + 1)]
    factor = jnp.sqrt(jnp.maximum(total, floor))[:, total.shape[1] - 1 :]
    pieces = sems.shape[0]
    size = near // pieces
    copies = []
    for i in range(pieces):
        for b in range(i * size, (i + 1) * size):
            begin = b * (rows + 1)
            buf[b * rows : (b + 1) * rows] = gathered[begin : begin + rows] * factor
        part = pl.ds(i * size * rows, size * rows)
        copies.append(pltpu.make_async_copy(buf.at[part], out.at[part], sems.at[i]))
        copies[-1].start()
    for copy in copies:
        copy.wait()


SMALL = pltpu.CompilerParams(vmem_limit_bytes=4 << 20)


def on_device(near_groups, far_groups, propagator, site_coords, momenta, source_slice):
    _, sinks, sources, _, slices, local_sites = propagator.shape
    pairs = sinks * sources
    lanes = 2 * momenta.shape[1]
    near = len(near_groups[0])
    far = len(far_groups[0])
    rows = pairs * slices // near
    all_sites = float(local_sites * lax.axis_size(SITE_AXES))
    blocks, picked = project(propagator, site_coords, momenta, source_slice, near)
    received = exchange(blocks.reshape(near, rows + 1, 1, lanes), SITE_AXES, near_groups)
    picked = lax.psum(picked, "ta")
    blocks = pl.pallas_call(
        functools.partial(near_kernel, near, far, slices),
        out_shape=jax.ShapeDtypeStruct((far * (rows + 1), lanes), jnp.float32),
        in_specs=[IN_VMEM] * 2,
        out_specs=IN_VMEM,
        compiler_params=SMALL,
    )(received.reshape(near * (rows + 1), lanes), picked)
    received = exchange(blocks.reshape(far, rows + 1, 1, lanes), "xy", far_groups)
    blocks = pl.pallas_call(
        functools.partial(far_kernel, near, far, slices, all_sites),
        out_shape=jax.ShapeDtypeStruct((near * (rows + 1), lanes), jnp.float32),
        in_specs=[IN_VMEM],
        out_specs=IN_VMEM,
        compiler_params=SMALL,
    )(received.reshape(far * (rows + 1), lanes))
    received = exchange(blocks.reshape(near, rows + 1, 1, lanes), SITE_AXES, near_groups)
    correlator = pl.pallas_call(
        functools.partial(scale_kernel, near, all_sites),
        out_shape=jax.ShapeDtypeStruct((near * rows, lanes), jnp.float32),
        in_specs=[IN_VMEM],
        out_specs=IN_HBM,
        scratch_shapes=[
            pltpu.VMEM((near * rows, lanes), jnp.float32),
            pltpu.SemaphoreType.DMA((2,)),
        ],
        compiler_params=SMALL,
    )(received.reshape(near * (rows + 1), lanes))
    return correlator.reshape(pairs, slices, lanes)


def solution(mesh):
    near_groups, far_groups = groups(mesh.shape["xy"], mesh.shape["gz"])
    return jax.shard_map(
        functools.partial(on_device, near_groups, far_groups),
        mesh=mesh,
        in_specs=(P(None, None, None, None, "ta", SITE_AXES), P(None, SITE_AXES), P(), P()),
        out_specs=P(None, "ta", None),
        check_vma=False,
    )
```

```python
import functools
import math

import jax
import jax.numpy as jnp
from jax import lax
from jax.experimental import pallas as pl
from jax.experimental.pallas import tpu as pltpu
from jax.sharding import PartitionSpec as P

EXTENT = 96
SITE_AXES = ("xy", "gz")
IN_HBM = pl.BlockSpec(memory_space=pltpu.HBM)
IN_VMEM = pl.BlockSpec(memory_space=pltpu.VMEM)


def groups(planes, blocks):
    pairs = planes // 2
    half = pairs // 2
    plane = []
    for p in range(pairs):
        swapped = (p % half == half // 4) != (p >= half)
        plane.append([2 * p + (m ^ swapped) for m in range(2)])
    alternate = [b for start in (0, blocks // 2) for b in range(start, start + blocks // 2)]
    alternate = [alternate[(i % 2) * (blocks // 2) + i // 2] for i in range(blocks)]
    cores = [b for core in range(2) for b in alternate if b % 2 == core]
    near = [[plane[p][m] * blocks + b for b in cores for m in range(2)] for p in range(pairs)]
    order = [*range(half, pairs), *reversed(range(half))]
    far = [[plane[p][m] for p in order] for m in range(2)]
    return near, far


def exchange(x, axes, axis_groups=None):
    return lax.all_to_all(
        x, axes, split_axis=0, concat_axis=0, tiled=True, axis_index_groups=axis_groups
    )


def phase_table(coords, momenta):
    both = jnp.concatenate([momenta, momenta], axis=1)
    turns = lax.dot_general(
        coords, both, (((0,), (0,)), ((), ())), preferred_element_type=jnp.float32
    )
    lane = lax.broadcasted_iota(jnp.int32, turns.shape, 1)
    turns = turns + jnp.where(lane >= momenta.shape[1], EXTENT / 4.0, 0.0)
    turns = turns - EXTENT * jnp.floor((turns + 0.5) * (1.0 / EXTENT))
    angle = (jnp.abs(turns - EXTENT / 2.0) - EXTENT / 4.0) * (2.0 * math.pi / EXTENT)
    square = angle * angle
    series = jnp.full_like(square, 1.0 / math.factorial(13))
    for power in (11, 9, 7, 5, 3, 1):
        sign = -1.0 if power % 4 == 3 else 1.0
        series = series * square + sign / math.factorial(power)
    return series * angle


def project_kernel(
    near, propagator, coords, momenta, source, out, parts, site_buf, mom_buf, src_buf, density,
    part_sem, small_sem,
):
    _, sinks, sources, colors, slices, _ = propagator.shape
    pairs = sinks * sources
    step = pairs // part_sem.shape[0]
    lanes = out.shape[1]
    rows = pairs * slices // near
    loads = [
        pltpu.make_async_copy(coords, site_buf, small_sem.at[0]),
        pltpu.make_async_copy(momenta, mom_buf, small_sem.at[1]),
        pltpu.make_async_copy(source, src_buf, small_sem.at[2]),
    ]
    for load in loads:
        load.start()
    copies = [
        pltpu.make_async_copy(
            propagator.at[:, p // sources, pl.ds(p % sources, step)],
            parts.at[:, pl.ds(p, step)],
            part_sem.at[p // step],
        )
        for p in range(0, pairs, step)
    ]
    for copy in copies:
        copy.start()
    for load in loads:
        load.wait()
    phases = phase_table(site_buf[...].astype(jnp.float32), mom_buf[...].astype(jnp.float32))
    first = lax.axis_index("ta") * slices
    row = lax.broadcasted_iota(jnp.int32, (slices, lanes), 0)
    lane = lax.broadcasted_iota(jnp.int32, (slices, lanes), 1)
    weight = jnp.zeros((slices, lanes), jnp.float32)
    for i in range(source.shape[0]):
        weight = weight + jnp.where(row == src_buf[i] - first, 1.0, 0.0)
    weight = jnp.where(lane < slices, jnp.where(row == lane, 1.0, 0.0), weight)
    over_pairs = None
    for p in range(pairs):
        if p % step == 0:
            copies[p // step].wait()
        value = None
        for r in range(2):
            for c in range(colors):
                part = parts[r, p, c]
                value = part * part if value is None else value + part * part
        density[p * slices : (p + 1) * slices] = value
        over_pairs = value if over_pairs is None else over_pairs + value
    by_slice = jnp.sum(over_pairs, axis=1, keepdims=True)
    stats = jnp.sum(by_slice * weight, axis=0, keepdims=True)
    projected = jnp.dot(
        density[...],
        phases,
        precision=lax.Precision.HIGHEST,
        preferred_element_type=jnp.float32,
    )
    for block in range(near):
        begin = block * (rows + 1)
        out[begin : begin + rows] = projected[block * rows : (block + 1) * rows]
        out[begin + rows : begin + rows + 1] = stats


def project(propagator, coords, momenta, source, near):
    _, sinks, sources, colors, slices, sites = propagator.shape
    pairs = sinks * sources
    lanes = 2 * momenta.shape[1]
    arrays = (propagator, coords, momenta, source)
    return pl.pallas_call(
        functools.partial(project_kernel, near),
        out_shape=jax.ShapeDtypeStruct((pairs * slices + near, lanes), jnp.float32),
        in_specs=[IN_HBM] * 4,
        out_specs=IN_VMEM,
        scratch_shapes=[
            pltpu.VMEM((2, pairs, colors, slices, sites), jnp.float32),
            pltpu.VMEM(coords.shape, jnp.int32),
            pltpu.VMEM(momenta.shape, jnp.int32),
            pltpu.SMEM(source.shape, jnp.int32),
            pltpu.VMEM((pairs * slices, sites), jnp.float32),
            pltpu.SemaphoreType.DMA((pairs // 2,)),
            pltpu.SemaphoreType.DMA((3,)),
        ],
        compiler_params=pltpu.CompilerParams(vmem_limit_bytes=12 << 20),
    )(*[pltpu.with_memory_space_constraint(x, pltpu.HBM) for x in arrays])


def sum_of_blocks(ref, blocks):
    rows = ref.shape[0] // blocks
    value = ref[:rows]
    for b in range(1, blocks):
        value = value + ref[b * rows : (b + 1) * rows]
    return value


def near_kernel(near, far, received, out):
    value = sum_of_blocks(received, near)
    rows = value.shape[0]
    for b in range(far):
        out[b * rows : (b + 1) * rows] = value


def far_kernel(far, slices, floor, received, out, picked):
    value = sum_of_blocks(received, far)
    rows = value.shape[0] - 1
    lanes = value.shape[1]
    stats = value[rows:]
    row = lax.broadcasted_iota(jnp.int32, (slices, lanes), 0)
    lane = lax.broadcasted_iota(jnp.int32, (slices, lanes), 1)
    column = jnp.sum(jnp.where(row == lane, stats, 0.0), axis=1, keepdims=True)
    norm = jnp.maximum(column, floor)
    for pair in range(rows // slices):
        scaled = value[pair * slices : (pair + 1) * slices] / norm
        for b in range(out.shape[0]):
            out[b, pair * slices : (pair + 1) * slices] = scaled
    picked[...] = stats


def scale_kernel(floor, gathered, total, out, buf, sems):
    factor = jnp.sqrt(jnp.maximum(total[...], floor))[:, out.shape[2] - 1 :]
    pieces = sems.shape[0]
    size = gathered.shape[0] // pieces
    copies = []
    for i in range(pieces):
        part = slice(i * size, (i + 1) * size)
        buf[part] = gathered[part] * factor[None]
        copies.append(pltpu.make_async_copy(buf.at[part], out.at[part], sems.at[i]))
        copies[-1].start()
    for copy in copies:
        copy.wait()


SMALL = pltpu.CompilerParams(vmem_limit_bytes=4 << 20)


def on_device(near_groups, far_groups, propagator, site_coords, momenta, source_slice):
    _, sinks, sources, _, slices, local_sites = propagator.shape
    pairs = sinks * sources
    lanes = 2 * momenta.shape[1]
    near = len(near_groups[0])
    far = len(far_groups[0])
    rows = pairs * slices // near
    all_sites = float(local_sites * lax.axis_size(SITE_AXES))
    blocks = project(propagator, site_coords, momenta, source_slice, near)
    received = exchange(blocks.reshape(near, rows + 1, 1, lanes), SITE_AXES, near_groups)
    blocks = pl.pallas_call(
        functools.partial(near_kernel, near, far),
        out_shape=jax.ShapeDtypeStruct((far * (rows + 1), lanes), jnp.float32),
        in_specs=[IN_VMEM],
        out_specs=IN_VMEM,
        compiler_params=SMALL,
    )(received.reshape(near * (rows + 1), lanes))
    received = exchange(blocks.reshape(far, rows + 1, 1, lanes), "xy", far_groups)
    scaled, picked = pl.pallas_call(
        functools.partial(far_kernel, far, slices, all_sites),
        out_shape=(
            jax.ShapeDtypeStruct((near, rows, lanes), jnp.float32),
            jax.ShapeDtypeStruct((1, lanes), jnp.float32),
        ),
        in_specs=[IN_VMEM],
        out_specs=(IN_VMEM, IN_VMEM),
        compiler_params=SMALL,
    )(received.reshape(far * (rows + 1), lanes))
    gathered = exchange(scaled, SITE_AXES, near_groups)
    picked = lax.psum(picked, "ta")
    correlator = pl.pallas_call(
        functools.partial(scale_kernel, all_sites),
        out_shape=jax.ShapeDtypeStruct((pairs, slices, lanes), jnp.float32),
        in_specs=[IN_VMEM] * 2,
        out_specs=pl.BlockSpec(memory_space=pltpu.HBM),
        scratch_shapes=[
            pltpu.VMEM((pairs, slices, lanes), jnp.float32),
            pltpu.SemaphoreType.DMA((2,)),
        ],
        compiler_params=SMALL,
    )(gathered.reshape(pairs, slices, lanes), picked)
    return correlator


def solution(mesh):
    near_groups, far_groups = groups(mesh.shape["xy"], mesh.shape["gz"])
    return jax.shard_map(
        functools.partial(on_device, near_groups, far_groups),
        mesh=mesh,
        in_specs=(P(None, None, None, None, "ta", SITE_AXES), P(None, SITE_AXES), P(), P()),
        out_specs=P(None, "ta", None),
        check_vma=False,
    )
```

```python
import functools
import math

import jax
import jax.numpy as jnp
from jax import lax
from jax.experimental import pallas as pl
from jax.experimental.pallas import tpu as pltpu
from jax.sharding import PartitionSpec as P

EXTENT = 96
SITE_AXES = ("xy", "gz")
IN_HBM = pl.BlockSpec(memory_space=pltpu.HBM)
IN_VMEM = pl.BlockSpec(memory_space=pltpu.VMEM)


NEAR_BLOCKS = (5, 4, 7, 6, 3, 2, 1, 0)
GATHER_BLOCKS = (3, 1, 7, 5, 0, 2, 6, 4)


def groups(planes, blocks):
    pairs = planes // 2
    half = pairs // 2
    plane = []
    for p in range(pairs):
        swapped = (p % half == half // 4) != (p >= half)
        plane.append([2 * p + (m ^ swapped) for m in range(2)])
    near = [[plane[p][m] * blocks + b for b in NEAR_BLOCKS for m in range(2)] for p in range(pairs)]
    gather = [[plane[p][m] * blocks + b for b in GATHER_BLOCKS for m in range(2)] for p in range(pairs)]
    order = [*range(half, pairs), *reversed(range(half))]
    far = [[plane[p][m] for p in order] for m in range(2)]
    return near, far, gather


def exchange(x, axes, axis_groups=None):
    return lax.all_to_all(
        x, axes, split_axis=0, concat_axis=0, tiled=True, axis_index_groups=axis_groups
    )


def phase_table(coords, momenta):
    both = jnp.concatenate([momenta, momenta], axis=1)
    turns = lax.dot_general(
        coords, both, (((0,), (0,)), ((), ())), preferred_element_type=jnp.float32
    )
    lane = lax.broadcasted_iota(jnp.int32, turns.shape, 1)
    turns = turns + jnp.where(lane >= momenta.shape[1], EXTENT / 4.0, 0.0)
    turns = turns - EXTENT * jnp.floor((turns + 0.5) * (1.0 / EXTENT))
    angle = (jnp.abs(turns - EXTENT / 2.0) - EXTENT / 4.0) * (2.0 * math.pi / EXTENT)
    square = angle * angle
    series = jnp.full_like(square, 1.0 / math.factorial(13))
    for power in (11, 9, 7, 5, 3, 1):
        sign = -1.0 if power % 4 == 3 else 1.0
        series = series * square + sign / math.factorial(power)
    return series * angle


def project_kernel(
    near, propagator, coords, momenta, source, out, parts, site_buf, mom_buf, src_buf, density,
    part_sem, small_sem,
):
    _, sinks, sources, colors, slices, _ = propagator.shape
    pairs = sinks * sources
    step = pairs // part_sem.shape[0]
    lanes = out.shape[1]
    rows = pairs * slices // near
    loads = [
        pltpu.make_async_copy(coords, site_buf, small_sem.at[0]),
        pltpu.make_async_copy(momenta, mom_buf, small_sem.at[1]),
        pltpu.make_async_copy(source, src_buf, small_sem.at[2]),
    ]
    for load in loads:
        load.start()
    copies = [
        pltpu.make_async_copy(
            propagator.at[:, p // sources, pl.ds(p % sources, step)],
            parts.at[:, pl.ds(p, step)],
            part_sem.at[p // step],
        )
        for p in range(0, pairs, step)
    ]
    for copy in copies:
        copy.start()
    for load in loads:
        load.wait()
    phases = phase_table(site_buf[...].astype(jnp.float32), mom_buf[...].astype(jnp.float32))
    first = lax.axis_index("ta") * slices
    row = lax.broadcasted_iota(jnp.int32, (slices, lanes), 0)
    lane = lax.broadcasted_iota(jnp.int32, (slices, lanes), 1)
    weight = jnp.zeros((slices, lanes), jnp.float32)
    for i in range(source.shape[0]):
        weight = weight + jnp.where(row == src_buf[i] - first, 1.0, 0.0)
    weight = jnp.where(lane < slices, jnp.where(row == lane, 1.0, 0.0), weight)
    over_pairs = None
    for p in range(pairs):
        if p % step == 0:
            copies[p // step].wait()
        value = None
        for r in range(2):
            for c in range(colors):
                part = parts[r, p, c]
                value = part * part if value is None else value + part * part
        density[p * slices : (p + 1) * slices] = value
        over_pairs = value if over_pairs is None else over_pairs + value
    by_slice = jnp.sum(over_pairs, axis=1, keepdims=True)
    stats = jnp.sum(by_slice * weight, axis=0, keepdims=True)
    projected = jnp.dot(
        density[...],
        phases,
        precision=lax.Precision.HIGHEST,
        preferred_element_type=jnp.float32,
    )
    for block in range(near):
        begin = block * (rows + 1)
        out[begin : begin + rows] = projected[block * rows : (block + 1) * rows]
        out[begin + rows : begin + rows + 1] = stats


def project(propagator, coords, momenta, source, near):
    _, sinks, sources, colors, slices, sites = propagator.shape
    pairs = sinks * sources
    lanes = 2 * momenta.shape[1]
    arrays = (propagator, coords, momenta, source)
    return pl.pallas_call(
        functools.partial(project_kernel, near),
        out_shape=jax.ShapeDtypeStruct((pairs * slices + near, lanes), jnp.float32),
        in_specs=[IN_HBM] * 4,
        out_specs=IN_VMEM,
        scratch_shapes=[
            pltpu.VMEM((2, pairs, colors, slices, sites), jnp.float32),
            pltpu.VMEM(coords.shape, jnp.int32),
            pltpu.VMEM(momenta.shape, jnp.int32),
            pltpu.SMEM(source.shape, jnp.int32),
            pltpu.VMEM((pairs * slices, sites), jnp.float32),
            pltpu.SemaphoreType.DMA((pairs // 2,)),
            pltpu.SemaphoreType.DMA((3,)),
        ],
        compiler_params=pltpu.CompilerParams(vmem_limit_bytes=12 << 20),
    )(*[pltpu.with_memory_space_constraint(x, pltpu.HBM) for x in arrays])


def sum_of_blocks(ref, blocks):
    rows = ref.shape[0] // blocks
    value = ref[:rows]
    for b in range(1, blocks):
        value = value + ref[b * rows : (b + 1) * rows]
    return value


def near_kernel(near, far, received, out):
    value = sum_of_blocks(received, near)
    rows = value.shape[0]
    for b in range(far):
        out[b * rows : (b + 1) * rows] = value


def far_kernel(far, slices, floor, received, out, picked):
    value = sum_of_blocks(received, far)
    rows = value.shape[0] - 1
    lanes = value.shape[1]
    stats = value[rows:]
    row = lax.broadcasted_iota(jnp.int32, (slices, lanes), 0)
    lane = lax.broadcasted_iota(jnp.int32, (slices, lanes), 1)
    column = jnp.sum(jnp.where(row == lane, stats, 0.0), axis=1, keepdims=True)
    norm = jnp.maximum(column, floor)
    for pair in range(rows // slices):
        scaled = value[pair * slices : (pair + 1) * slices] / norm
        for b in range(out.shape[0]):
            out[b, pair * slices : (pair + 1) * slices] = scaled
    picked[...] = stats


def scale_kernel(places, floor, gathered, total, out, buf, sems):
    total = jnp.sum(total[...], axis=0, keepdims=True)
    factor = jnp.sqrt(jnp.maximum(total, floor))[:, total.shape[1] - 1 :]
    rows = gathered.shape[1]
    for slot, place in enumerate(places):
        buf[place * rows : (place + 1) * rows] = gathered[slot] * factor
    size = buf.shape[0] // sems.shape[0]
    copies = [
        pltpu.make_async_copy(
            buf.at[pl.ds(i * size, size)], out.at[pl.ds(i * size, size)], sems.at[i]
        )
        for i in range(sems.shape[0])
    ]
    for copy in copies:
        copy.start()
    for copy in copies:
        copy.wait()


SMALL = pltpu.CompilerParams(vmem_limit_bytes=4 << 20)


def on_device(near_groups, far_groups, gather_groups, propagator, site_coords, momenta, source_slice):
    _, sinks, sources, _, slices, local_sites = propagator.shape
    pairs = sinks * sources
    lanes = 2 * momenta.shape[1]
    near = len(near_groups[0])
    far = len(far_groups[0])
    rows = pairs * slices // near
    all_sites = float(local_sites * lax.axis_size(SITE_AXES))
    blocks = project(propagator, site_coords, momenta, source_slice, near)
    received = exchange(blocks.reshape(near, rows + 1, 1, lanes), SITE_AXES, near_groups)
    blocks = pl.pallas_call(
        functools.partial(near_kernel, near, far),
        out_shape=jax.ShapeDtypeStruct((far * (rows + 1), lanes), jnp.float32),
        in_specs=[IN_VMEM],
        out_specs=IN_VMEM,
        compiler_params=SMALL,
    )(received.reshape(near * (rows + 1), lanes))
    received = exchange(blocks.reshape(far, rows + 1, 1, lanes), "xy", far_groups)
    scaled, picked = pl.pallas_call(
        functools.partial(far_kernel, far, slices, all_sites),
        out_shape=(
            jax.ShapeDtypeStruct((near, rows, lanes), jnp.float32),
            jax.ShapeDtypeStruct((1, lanes), jnp.float32),
        ),
        in_specs=[IN_VMEM],
        out_specs=(IN_VMEM, IN_VMEM),
        compiler_params=SMALL,
    )(received.reshape(far * (rows + 1), lanes))
    gathered = exchange(scaled, SITE_AXES, gather_groups)
    picked = lax.all_gather(picked, "ta", axis=0, tiled=True)
    places = [near_groups[0].index(member) for member in gather_groups[0]]
    correlator = pl.pallas_call(
        functools.partial(scale_kernel, places, all_sites),
        out_shape=jax.ShapeDtypeStruct((near * rows, lanes), jnp.float32),
        in_specs=[IN_VMEM] * 2,
        out_specs=IN_HBM,
        scratch_shapes=[
            pltpu.VMEM((near * rows, lanes), jnp.float32),
            pltpu.SemaphoreType.DMA((2,)),
        ],
        compiler_params=SMALL,
    )(gathered, picked)
    return correlator.reshape(pairs, slices, lanes)


def solution(mesh):
    near_groups, far_groups, gather_groups = groups(mesh.shape["xy"], mesh.shape["gz"])
    return jax.shard_map(
        functools.partial(on_device, near_groups, far_groups, gather_groups),
        mesh=mesh,
        in_specs=(P(None, None, None, None, "ta", SITE_AXES), P(None, SITE_AXES), P(), P()),
        out_specs=P(None, "ta", None),
        check_vma=False,
    )
```

```python
import functools
import math

import jax
import jax.numpy as jnp
from jax import lax
from jax.experimental import pallas as pl
from jax.experimental.pallas import tpu as pltpu
from jax.sharding import PartitionSpec as P

EXTENT = 96
SITE_AXES = ("xy", "gz")
IN_HBM = pl.BlockSpec(memory_space=pltpu.HBM)
IN_VMEM = pl.BlockSpec(memory_space=pltpu.VMEM)


NEAR_BLOCKS = (5, 4, 7, 6, 3, 2, 1, 0)
GATHER_BLOCKS = (3, 1, 7, 5, 0, 2, 6, 4)


def groups(planes, blocks):
    pairs = planes // 2
    half = pairs // 2
    plane = []
    for p in range(pairs):
        swapped = (p % half == half // 4) != (p >= half)
        plane.append([2 * p + (m ^ swapped) for m in range(2)])
    near = [[plane[p][m] * blocks + b for b in NEAR_BLOCKS for m in range(2)] for p in range(pairs)]
    gather = [[plane[p][m] * blocks + b for b in GATHER_BLOCKS for m in range(2)] for p in range(pairs)]
    order = [*range(half, pairs), *reversed(range(half))]
    far = [[plane[p][m] for p in order] for m in range(2)]
    return near, far, gather


def exchange(x, axes, axis_groups=None):
    return lax.all_to_all(
        x, axes, split_axis=0, concat_axis=0, tiled=True, axis_index_groups=axis_groups
    )


def phase_table(coords, momenta):
    both = jnp.concatenate([momenta, momenta], axis=1)
    turns = lax.dot_general(
        coords, both, (((0,), (0,)), ((), ())), preferred_element_type=jnp.float32
    )
    lane = lax.broadcasted_iota(jnp.int32, turns.shape, 1)
    turns = turns + jnp.where(lane >= momenta.shape[1], EXTENT / 4.0, 0.0)
    turns = turns - EXTENT * jnp.floor((turns + 0.5) * (1.0 / EXTENT))
    angle = (jnp.abs(turns - EXTENT / 2.0) - EXTENT / 4.0) * (2.0 * math.pi / EXTENT)
    square = angle * angle
    series = jnp.full_like(square, 1.0 / math.factorial(13))
    for power in (11, 9, 7, 5, 3, 1):
        sign = -1.0 if power % 4 == 3 else 1.0
        series = series * square + sign / math.factorial(power)
    return series * angle


def project_kernel(
    near, propagator, coords, momenta, source, out, parts, site_buf, mom_buf, src_buf, density,
    part_sem, small_sem,
):
    _, sinks, sources, colors, slices, _ = propagator.shape
    pairs = sinks * sources
    step = pairs // part_sem.shape[0]
    lanes = out.shape[1]
    rows = pairs * slices // near
    loads = [
        pltpu.make_async_copy(coords, site_buf, small_sem.at[0]),
        pltpu.make_async_copy(momenta, mom_buf, small_sem.at[1]),
        pltpu.make_async_copy(source, src_buf, small_sem.at[2]),
    ]
    for load in loads:
        load.start()
    copies = [
        pltpu.make_async_copy(
            propagator.at[:, p // sources, pl.ds(p % sources, step)],
            parts.at[:, pl.ds(p, step)],
            part_sem.at[p // step],
        )
        for p in range(0, pairs, step)
    ]
    for copy in copies:
        copy.start()
    for load in loads:
        load.wait()
    phases = phase_table(site_buf[...].astype(jnp.float32), mom_buf[...].astype(jnp.float32))
    first = lax.axis_index("ta") * slices
    row = lax.broadcasted_iota(jnp.int32, (slices, lanes), 0)
    lane = lax.broadcasted_iota(jnp.int32, (slices, lanes), 1)
    weight = jnp.zeros((slices, lanes), jnp.float32)
    for i in range(source.shape[0]):
        weight = weight + jnp.where(row == src_buf[i] - first, 1.0, 0.0)
    weight = jnp.where(lane < slices, jnp.where(row == lane, 1.0, 0.0), weight)
    over_pairs = None
    for p in range(pairs):
        if p % step == 0:
            copies[p // step].wait()
        value = None
        for r in range(2):
            for c in range(colors):
                part = parts[r, p, c]
                value = part * part if value is None else value + part * part
        density[p * slices : (p + 1) * slices] = value
        over_pairs = value if over_pairs is None else over_pairs + value
    by_slice = jnp.sum(over_pairs, axis=1, keepdims=True)
    stats = jnp.sum(by_slice * weight, axis=0, keepdims=True)
    projected = jnp.dot(
        density[...],
        phases,
        precision=lax.Precision.HIGHEST,
        preferred_element_type=jnp.float32,
    )
    for block in range(near):
        begin = block * (rows + 1)
        out[begin : begin + rows] = projected[block * rows : (block + 1) * rows]
        out[begin + rows : begin + rows + 1] = stats


def project(propagator, coords, momenta, source, near):
    _, sinks, sources, colors, slices, sites = propagator.shape
    pairs = sinks * sources
    lanes = 2 * momenta.shape[1]
    arrays = (propagator, coords, momenta, source)
    return pl.pallas_call(
        functools.partial(project_kernel, near),
        out_shape=jax.ShapeDtypeStruct((pairs * slices + near, lanes), jnp.float32),
        in_specs=[IN_HBM] * 4,
        out_specs=IN_VMEM,
        scratch_shapes=[
            pltpu.VMEM((2, pairs, colors, slices, sites), jnp.float32),
            pltpu.VMEM(coords.shape, jnp.int32),
            pltpu.VMEM(momenta.shape, jnp.int32),
            pltpu.SMEM(source.shape, jnp.int32),
            pltpu.VMEM((pairs * slices, sites), jnp.float32),
            pltpu.SemaphoreType.DMA((pairs // 2,)),
            pltpu.SemaphoreType.DMA((3,)),
        ],
        compiler_params=pltpu.CompilerParams(vmem_limit_bytes=12 << 20),
    )(*[pltpu.with_memory_space_constraint(x, pltpu.HBM) for x in arrays])


def sum_of_blocks(ref, blocks):
    rows = ref.shape[0] // blocks
    value = ref[:rows]
    for b in range(1, blocks):
        value = value + ref[b * rows : (b + 1) * rows]
    return value


def near_kernel(near, far, received, out):
    value = sum_of_blocks(received, near)
    rows = value.shape[0]
    for b in range(far):
        out[b * rows : (b + 1) * rows] = value


def far_kernel(far, slices, floor, received, out, picked):
    value = sum_of_blocks(received, far)
    rows = value.shape[0] - 1
    lanes = value.shape[1]
    stats = value[rows:]
    row = lax.broadcasted_iota(jnp.int32, (slices, lanes), 0)
    lane = lax.broadcasted_iota(jnp.int32, (slices, lanes), 1)
    column = jnp.sum(jnp.where(row == lane, stats, 0.0), axis=1, keepdims=True)
    norm = jnp.maximum(column, floor)
    for pair in range(rows // slices):
        scaled = value[pair * slices : (pair + 1) * slices] / norm
        for b in range(out.shape[0]):
            out[b, pair * slices : (pair + 1) * slices] = scaled
    picked[...] = stats


def scale_kernel(places, floor, gathered, total, out, buf, sems):
    total = jnp.sum(total[...], axis=0, keepdims=True)
    factor = jnp.sqrt(jnp.maximum(total, floor))[:, total.shape[1] - 1 :]
    rows = gathered.shape[1]
    for slot, place in enumerate(places):
        buf[place * rows : (place + 1) * rows] = gathered[slot] * factor
    size = buf.shape[0] // sems.shape[0]
    copies = [
        pltpu.make_async_copy(
            buf.at[pl.ds(i * size, size)], out.at[pl.ds(i * size, size)], sems.at[i]
        )
        for i in range(sems.shape[0])
    ]
    for copy in copies:
        copy.start()
    for copy in copies:
        copy.wait()


SMALL = pltpu.CompilerParams(vmem_limit_bytes=4 << 20)


def on_device(near_groups, far_groups, gather_groups, propagator, site_coords, momenta, source_slice):
    _, sinks, sources, _, slices, local_sites = propagator.shape
    pairs = sinks * sources
    lanes = 2 * momenta.shape[1]
    near = len(near_groups[0])
    far = len(far_groups[0])
    rows = pairs * slices // near
    all_sites = float(local_sites * lax.axis_size(SITE_AXES))
    blocks = project(propagator, site_coords, momenta, source_slice, near)
    received = exchange(blocks.reshape(near, rows + 1, 1, lanes), SITE_AXES, near_groups)
    blocks = pl.pallas_call(
        functools.partial(near_kernel, near, far),
        out_shape=jax.ShapeDtypeStruct((far * (rows + 1), lanes), jnp.float32),
        in_specs=[IN_VMEM],
        out_specs=IN_VMEM,
        compiler_params=SMALL,
    )(received.reshape(near * (rows + 1), lanes))
    received = exchange(blocks.reshape(far, rows + 1, 1, lanes), "xy", far_groups)
    scaled, picked = pl.pallas_call(
        functools.partial(far_kernel, far, slices, all_sites),
        out_shape=(
            jax.ShapeDtypeStruct((near, rows, lanes), jnp.float32),
            jax.ShapeDtypeStruct((1, lanes), jnp.float32),
        ),
        in_specs=[IN_VMEM],
        out_specs=(IN_VMEM, IN_VMEM),
        compiler_params=SMALL,
    )(received.reshape(far * (rows + 1), lanes))
    gathered = exchange(scaled, SITE_AXES, gather_groups)
    picked = lax.all_gather(
        picked,
        "ta",
        axis=0,
        tiled=True,
        axis_index_groups=[[*reversed(range(lax.axis_size("ta")))]],
    )
    places = [near_groups[0].index(member) for member in gather_groups[0]]
    correlator = pl.pallas_call(
        functools.partial(scale_kernel, places, all_sites),
        out_shape=jax.ShapeDtypeStruct((near * rows, lanes), jnp.float32),
        in_specs=[IN_VMEM] * 2,
        out_specs=IN_HBM,
        scratch_shapes=[
            pltpu.VMEM((near * rows, lanes), jnp.float32),
            pltpu.SemaphoreType.DMA((2,)),
        ],
        compiler_params=SMALL,
    )(gathered, picked)
    return correlator.reshape(pairs, slices, lanes)


def solution(mesh):
    near_groups, far_groups, gather_groups = groups(mesh.shape["xy"], mesh.shape["gz"])
    return jax.shard_map(
        functools.partial(on_device, near_groups, far_groups, gather_groups),
        mesh=mesh,
        in_specs=(P(None, None, None, None, "ta", SITE_AXES), P(None, SITE_AXES), P(), P()),
        out_specs=P(None, "ta", None),
        check_vma=False,
    )
```

```python
import functools
import math

import jax
import jax.numpy as jnp
from jax import lax
from jax.experimental import pallas as pl
from jax.experimental.pallas import tpu as pltpu
from jax.sharding import PartitionSpec as P

EXTENT = 96
SITE_AXES = ("xy", "gz")
IN_HBM = pl.BlockSpec(memory_space=pltpu.HBM)
IN_VMEM = pl.BlockSpec(memory_space=pltpu.VMEM)


NEAR_BLOCKS = (5, 4, 7, 6, 3, 2, 1, 0)
GATHER_BLOCKS = (3, 2, 1, 0, 5, 4, 7, 6)


def groups(planes, blocks):
    pairs = planes // 2
    half = pairs // 2
    plane = []
    for p in range(pairs):
        swapped = (p % half == half // 4) != (p >= half)
        plane.append([2 * p + (m ^ swapped) for m in range(2)])
    near = [[plane[p][m] * blocks + b for b in NEAR_BLOCKS for m in range(2)] for p in range(pairs)]
    gather = [[plane[p][m] * blocks + b for b in GATHER_BLOCKS for m in range(2)] for p in range(pairs)]
    late = half + 1
    order = [late, *(p for p in reversed(range(pairs)) if p != late)]
    far = [[plane[p][m] for p in order] for m in range(2)]
    return near, far, gather


def exchange(x, axes, axis_groups=None):
    return lax.all_to_all(
        x, axes, split_axis=0, concat_axis=0, tiled=True, axis_index_groups=axis_groups
    )


def phase_table(coords, momenta):
    both = jnp.concatenate([momenta, momenta], axis=1)
    turns = lax.dot_general(
        coords, both, (((0,), (0,)), ((), ())), preferred_element_type=jnp.float32
    )
    lane = lax.broadcasted_iota(jnp.int32, turns.shape, 1)
    turns = turns + jnp.where(lane >= momenta.shape[1], EXTENT / 4.0, 0.0)
    turns = turns - EXTENT * jnp.floor((turns + 0.5) * (1.0 / EXTENT))
    angle = (jnp.abs(turns - EXTENT / 2.0) - EXTENT / 4.0) * (2.0 * math.pi / EXTENT)
    square = angle * angle
    series = jnp.full_like(square, 1.0 / math.factorial(13))
    for power in (11, 9, 7, 5, 3, 1):
        sign = -1.0 if power % 4 == 3 else 1.0
        series = series * square + sign / math.factorial(power)
    return series * angle


def project_kernel(
    near, propagator, coords, momenta, source, out, parts, site_buf, mom_buf, src_buf, density,
    part_sem, small_sem,
):
    _, sinks, sources, colors, slices, _ = propagator.shape
    pairs = sinks * sources
    step = pairs // part_sem.shape[0]
    lanes = out.shape[1]
    rows = pairs * slices // near
    loads = [
        pltpu.make_async_copy(coords, site_buf, small_sem.at[0]),
        pltpu.make_async_copy(momenta, mom_buf, small_sem.at[1]),
        pltpu.make_async_copy(source, src_buf, small_sem.at[2]),
    ]
    for load in loads:
        load.start()
    copies = [
        pltpu.make_async_copy(
            propagator.at[:, p // sources, pl.ds(p % sources, step)],
            parts.at[:, pl.ds(p, step)],
            part_sem.at[p // step],
        )
        for p in range(0, pairs, step)
    ]
    for copy in copies:
        copy.start()
    for load in loads:
        load.wait()
    phases = phase_table(site_buf[...].astype(jnp.float32), mom_buf[...].astype(jnp.float32))
    first = lax.axis_index("ta") * slices
    row = lax.broadcasted_iota(jnp.int32, (slices, lanes), 0)
    lane = lax.broadcasted_iota(jnp.int32, (slices, lanes), 1)
    weight = jnp.zeros((slices, lanes), jnp.float32)
    for i in range(source.shape[0]):
        weight = weight + jnp.where(row == src_buf[i] - first, 1.0, 0.0)
    weight = jnp.where(lane < slices, jnp.where(row == lane, 1.0, 0.0), weight)
    over_pairs = None
    for p in range(pairs):
        if p % step == 0:
            copies[p // step].wait()
        value = None
        for r in range(2):
            for c in range(colors):
                part = parts[r, p, c]
                value = part * part if value is None else value + part * part
        density[p * slices : (p + 1) * slices] = value
        over_pairs = value if over_pairs is None else over_pairs + value
    by_slice = jnp.sum(over_pairs, axis=1, keepdims=True)
    stats = jnp.sum(by_slice * weight, axis=0, keepdims=True)
    projected = jnp.dot(
        density[...],
        phases,
        precision=lax.Precision.HIGHEST,
        preferred_element_type=jnp.float32,
    )
    for block in range(near):
        begin = block * (rows + 1)
        out[begin : begin + rows] = projected[block * rows : (block + 1) * rows]
        out[begin + rows : begin + rows + 1] = stats


def project(propagator, coords, momenta, source, near):
    _, sinks, sources, colors, slices, sites = propagator.shape
    pairs = sinks * sources
    lanes = 2 * momenta.shape[1]
    arrays = (propagator, coords, momenta, source)
    return pl.pallas_call(
        functools.partial(project_kernel, near),
        out_shape=jax.ShapeDtypeStruct((pairs * slices + near, lanes), jnp.float32),
        in_specs=[IN_HBM] * 4,
        out_specs=IN_VMEM,
        scratch_shapes=[
            pltpu.VMEM((2, pairs, colors, slices, sites), jnp.float32),
            pltpu.VMEM(coords.shape, jnp.int32),
            pltpu.VMEM(momenta.shape, jnp.int32),
            pltpu.SMEM(source.shape, jnp.int32),
            pltpu.VMEM((pairs * slices, sites), jnp.float32),
            pltpu.SemaphoreType.DMA((pairs // 2,)),
            pltpu.SemaphoreType.DMA((3,)),
        ],
        compiler_params=pltpu.CompilerParams(vmem_limit_bytes=12 << 20),
    )(*[pltpu.with_memory_space_constraint(x, pltpu.HBM) for x in arrays])


def sum_of_blocks(ref, blocks):
    rows = ref.shape[0] // blocks
    value = ref[:rows]
    for b in range(1, blocks):
        value = value + ref[b * rows : (b + 1) * rows]
    return value


def near_kernel(near, far, received, out):
    value = sum_of_blocks(received, near)
    rows = value.shape[0]
    for b in range(far):
        out[b * rows : (b + 1) * rows] = value


def far_kernel(far, slices, floor, received, out, picked):
    value = sum_of_blocks(received, far)
    rows = value.shape[0] - 1
    lanes = value.shape[1]
    stats = value[rows:]
    row = lax.broadcasted_iota(jnp.int32, (slices, lanes), 0)
    lane = lax.broadcasted_iota(jnp.int32, (slices, lanes), 1)
    column = jnp.sum(jnp.where(row == lane, stats, 0.0), axis=1, keepdims=True)
    norm = jnp.maximum(column, floor)
    for pair in range(rows // slices):
        scaled = value[pair * slices : (pair + 1) * slices] / norm
        for b in range(out.shape[0]):
            out[b, pair * slices : (pair + 1) * slices] = scaled
    picked[...] = stats


def scale_kernel(places, floor, gathered, total, out, buf, sems):
    total = jnp.sum(total[...], axis=0, keepdims=True)
    factor = jnp.sqrt(jnp.maximum(total, floor))[:, total.shape[1] - 1 :]
    rows = gathered.shape[1]
    for slot, place in enumerate(places):
        buf[place * rows : (place + 1) * rows] = gathered[slot] * factor
    size = buf.shape[0] // sems.shape[0]
    copies = [
        pltpu.make_async_copy(
            buf.at[pl.ds(i * size, size)], out.at[pl.ds(i * size, size)], sems.at[i]
        )
        for i in range(sems.shape[0])
    ]
    for copy in copies:
        copy.start()
    for copy in copies:
        copy.wait()


SMALL = pltpu.CompilerParams(vmem_limit_bytes=4 << 20)


def on_device(near_groups, far_groups, gather_groups, propagator, site_coords, momenta, source_slice):
    _, sinks, sources, _, slices, local_sites = propagator.shape
    pairs = sinks * sources
    lanes = 2 * momenta.shape[1]
    near = len(near_groups[0])
    far = len(far_groups[0])
    rows = pairs * slices // near
    all_sites = float(local_sites * lax.axis_size(SITE_AXES))
    blocks = project(propagator, site_coords, momenta, source_slice, near)
    received = exchange(blocks.reshape(near, rows + 1, 1, lanes), SITE_AXES, near_groups)
    blocks = pl.pallas_call(
        functools.partial(near_kernel, near, far),
        out_shape=jax.ShapeDtypeStruct((far * (rows + 1), lanes), jnp.float32),
        in_specs=[IN_VMEM],
        out_specs=IN_VMEM,
        compiler_params=SMALL,
    )(received.reshape(near * (rows + 1), lanes))
    received = exchange(blocks.reshape(far, rows + 1, 1, lanes), "xy", far_groups)
    scaled, picked = pl.pallas_call(
        functools.partial(far_kernel, far, slices, all_sites),
        out_shape=(
            jax.ShapeDtypeStruct((near, rows, lanes), jnp.float32),
            jax.ShapeDtypeStruct((1, lanes), jnp.float32),
        ),
        in_specs=[IN_VMEM],
        out_specs=(IN_VMEM, IN_VMEM),
        compiler_params=SMALL,
    )(received.reshape(far * (rows + 1), lanes))
    gathered = exchange(scaled, SITE_AXES, gather_groups)
    picked = lax.all_gather(
        picked,
        "ta",
        axis=0,
        tiled=True,
        axis_index_groups=[[(1 - t) % lax.axis_size("ta") for t in range(lax.axis_size("ta"))]],
    )
    places = [near_groups[0].index(member) for member in gather_groups[0]]
    correlator = pl.pallas_call(
        functools.partial(scale_kernel, places, all_sites),
        out_shape=jax.ShapeDtypeStruct((near * rows, lanes), jnp.float32),
        in_specs=[IN_VMEM] * 2,
        out_specs=IN_HBM,
        scratch_shapes=[
            pltpu.VMEM((near * rows, lanes), jnp.float32),
            pltpu.SemaphoreType.DMA((2,)),
        ],
        compiler_params=SMALL,
    )(gathered, picked)
    return correlator.reshape(pairs, slices, lanes)


def solution(mesh):
    near_groups, far_groups, gather_groups = groups(mesh.shape["xy"], mesh.shape["gz"])
    return jax.shard_map(
        functools.partial(on_device, near_groups, far_groups, gather_groups),
        mesh=mesh,
        in_specs=(P(None, None, None, None, "ta", SITE_AXES), P(None, SITE_AXES), P(), P()),
        out_specs=P(None, "ta", None),
        check_vma=False,
    )
```

```python
import functools
import math

import jax
import jax.numpy as jnp
from jax import lax
from jax.experimental import pallas as pl
from jax.experimental.pallas import tpu as pltpu
from jax.sharding import PartitionSpec as P

EXTENT = 96
SITE_AXES = ("xy", "gz")
IN_HBM = pl.BlockSpec(memory_space=pltpu.HBM)
IN_VMEM = pl.BlockSpec(memory_space=pltpu.VMEM)


NEAR_BLOCKS = (5, 4, 7, 6, 3, 2, 1, 0)
GATHER_BLOCKS = (3, 2, 1, 0, 5, 4, 7, 6)


def groups(planes, blocks):
    pairs = planes // 2
    half = pairs // 2
    plane = []
    for p in range(pairs):
        swapped = (p % half == half // 4) != (p >= half)
        plane.append([2 * p + (m ^ swapped) for m in range(2)])
    near = [[plane[p][m] * blocks + b for b in NEAR_BLOCKS for m in range(2)] for p in range(pairs)]
    gather = [[plane[p][m] * blocks + b for b in GATHER_BLOCKS for m in range(2)] for p in range(pairs)]
    late = half + 1
    order = [late, *(p for p in reversed(range(pairs)) if p != late)]
    far = [[plane[p][m] for p in order] for m in range(2)]
    return near, far, gather


def exchange(x, axes, axis_groups=None):
    return lax.all_to_all(
        x, axes, split_axis=0, concat_axis=0, tiled=True, axis_index_groups=axis_groups
    )


def phase_table(coords, momenta):
    both = jnp.concatenate([momenta, momenta], axis=1)
    turns = lax.dot_general(
        coords, both, (((0,), (0,)), ((), ())), preferred_element_type=jnp.float32
    )
    lane = lax.broadcasted_iota(jnp.int32, turns.shape, 1)
    turns = turns + jnp.where(lane >= momenta.shape[1], EXTENT / 4.0, 0.0)
    turns = turns - EXTENT * jnp.floor((turns + 0.5) * (1.0 / EXTENT))
    angle = (jnp.abs(turns - EXTENT / 2.0) - EXTENT / 4.0) * (2.0 * math.pi / EXTENT)
    square = angle * angle
    series = jnp.full_like(square, 1.0 / math.factorial(13))
    for power in (11, 9, 7, 5, 3, 1):
        sign = -1.0 if power % 4 == 3 else 1.0
        series = series * square + sign / math.factorial(power)
    return series * angle


def project_kernel(
    near, propagator, coords, momenta, source, out, parts, site_buf, mom_buf, src_buf, density,
    part_sem, small_sem,
):
    _, sinks, sources, colors, slices, _ = propagator.shape
    pairs = sinks * sources
    step = pairs // part_sem.shape[0]
    lanes = out.shape[1]
    rows = pairs * slices // near
    loads = [
        pltpu.make_async_copy(coords, site_buf, small_sem.at[0]),
        pltpu.make_async_copy(momenta, mom_buf, small_sem.at[1]),
        pltpu.make_async_copy(source, src_buf, small_sem.at[2]),
    ]
    for load in loads:
        load.start()
    copies = [
        pltpu.make_async_copy(
            propagator.at[:, p // sources, pl.ds(p % sources, step)],
            parts.at[:, pl.ds(p, step)],
            part_sem.at[p // step],
        )
        for p in range(0, pairs, step)
    ]
    for copy in copies:
        copy.start()
    for load in loads:
        load.wait()
    phases = phase_table(site_buf[...].astype(jnp.float32), mom_buf[...].astype(jnp.float32))
    first = lax.axis_index("ta") * slices
    row = lax.broadcasted_iota(jnp.int32, (slices, lanes), 0)
    lane = lax.broadcasted_iota(jnp.int32, (slices, lanes), 1)
    weight = jnp.zeros((slices, lanes), jnp.float32)
    for i in range(source.shape[0]):
        weight = weight + jnp.where(row == src_buf[i] - first, 1.0, 0.0)
    weight = jnp.where(lane < slices, jnp.where(row == lane, 1.0, 0.0), weight)
    over_pairs = None
    for p in range(pairs):
        if p % step == 0:
            copies[p // step].wait()
        value = None
        for r in range(2):
            for c in range(colors):
                part = parts[r, p, c]
                value = part * part if value is None else value + part * part
        density[p * slices : (p + 1) * slices] = value
        over_pairs = value if over_pairs is None else over_pairs + value
    by_slice = jnp.sum(over_pairs, axis=1, keepdims=True)
    stats = jnp.sum(by_slice * weight, axis=0, keepdims=True)
    projected = jnp.dot(
        density[...],
        phases,
        precision=lax.Precision.HIGHEST,
        preferred_element_type=jnp.float32,
    )
    for block in range(near):
        begin = block * (rows + 1)
        out[begin : begin + rows] = projected[block * rows : (block + 1) * rows]
        out[begin + rows : begin + rows + 1] = stats


def project(propagator, coords, momenta, source, near):
    _, sinks, sources, colors, slices, sites = propagator.shape
    pairs = sinks * sources
    lanes = 2 * momenta.shape[1]
    arrays = (propagator, coords, momenta, source)
    return pl.pallas_call(
        functools.partial(project_kernel, near),
        out_shape=jax.ShapeDtypeStruct((pairs * slices + near, lanes), jnp.float32),
        in_specs=[IN_HBM] * 4,
        out_specs=IN_VMEM,
        scratch_shapes=[
            pltpu.VMEM((2, pairs, colors, slices, sites), jnp.float32),
            pltpu.VMEM(coords.shape, jnp.int32),
            pltpu.VMEM(momenta.shape, jnp.int32),
            pltpu.SMEM(source.shape, jnp.int32),
            pltpu.VMEM((pairs * slices, sites), jnp.float32),
            pltpu.SemaphoreType.DMA((pairs // 2,)),
            pltpu.SemaphoreType.DMA((3,)),
        ],
        compiler_params=pltpu.CompilerParams(vmem_limit_bytes=12 << 20),
    )(*[pltpu.with_memory_space_constraint(x, pltpu.HBM) for x in arrays])


def sum_of_blocks(ref, blocks):
    rows = ref.shape[0] // blocks
    value = ref[:rows]
    for b in range(1, blocks):
        value = value + ref[b * rows : (b + 1) * rows]
    return value


def near_kernel(near, far, received, out):
    value = sum_of_blocks(received, near)
    rows = value.shape[0]
    for b in range(far):
        out[b * rows : (b + 1) * rows] = value


def far_kernel(far, slices, floor, received, out, picked):
    value = sum_of_blocks(received, far)
    rows = value.shape[0] - 1
    lanes = value.shape[1]
    stats = value[rows:]
    row = lax.broadcasted_iota(jnp.int32, (slices, lanes), 0)
    lane = lax.broadcasted_iota(jnp.int32, (slices, lanes), 1)
    column = jnp.sum(jnp.where(row == lane, stats, 0.0), axis=1, keepdims=True)
    norm = jnp.maximum(column, floor)
    for pair in range(rows // slices):
        scaled = value[pair * slices : (pair + 1) * slices] / norm
        for b in range(out.shape[0]):
            out[b, pair * slices : (pair + 1) * slices] = scaled
    picked[...] = stats


def scale_kernel(places, floor, gathered, total, out, buf, sems):
    total = jnp.sum(total[...], axis=0, keepdims=True)
    factor = jnp.sqrt(jnp.maximum(total, floor))[:, total.shape[1] - 1 :]
    rows = gathered.shape[1]
    size = buf.shape[0] // sems.shape[0]
    copies = []
    for place in range(len(places)):
        buf[place * rows : (place + 1) * rows] = gathered[places.index(place)] * factor
        if (place + 1) * rows % size == 0:
            part = pl.ds(len(copies) * size, size)
            copies.append(
                pltpu.make_async_copy(buf.at[part], out.at[part], sems.at[len(copies)])
            )
            copies[-1].start()
    for copy in copies:
        copy.wait()


SMALL = pltpu.CompilerParams(vmem_limit_bytes=4 << 20)


def on_device(near_groups, far_groups, gather_groups, propagator, site_coords, momenta, source_slice):
    _, sinks, sources, _, slices, local_sites = propagator.shape
    pairs = sinks * sources
    lanes = 2 * momenta.shape[1]
    near = len(near_groups[0])
    far = len(far_groups[0])
    rows = pairs * slices // near
    all_sites = float(local_sites * lax.axis_size(SITE_AXES))
    blocks = project(propagator, site_coords, momenta, source_slice, near)
    received = exchange(blocks.reshape(near, rows + 1, 1, lanes), SITE_AXES, near_groups)
    blocks = pl.pallas_call(
        functools.partial(near_kernel, near, far),
        out_shape=jax.ShapeDtypeStruct((far * (rows + 1), lanes), jnp.float32),
        in_specs=[IN_VMEM],
        out_specs=IN_VMEM,
        compiler_params=SMALL,
    )(received.reshape(near * (rows + 1), lanes))
    received = exchange(blocks.reshape(far, rows + 1, 1, lanes), "xy", far_groups)
    scaled, picked = pl.pallas_call(
        functools.partial(far_kernel, far, slices, all_sites),
        out_shape=(
            jax.ShapeDtypeStruct((near, rows, lanes), jnp.float32),
            jax.ShapeDtypeStruct((1, lanes), jnp.float32),
        ),
        in_specs=[IN_VMEM],
        out_specs=(IN_VMEM, IN_VMEM),
        compiler_params=SMALL,
    )(received.reshape(far * (rows + 1), lanes))
    gathered = exchange(scaled, SITE_AXES, gather_groups)
    picked = lax.all_gather(
        picked,
        "ta",
        axis=0,
        tiled=True,
        axis_index_groups=[[(1 - t) % lax.axis_size("ta") for t in range(lax.axis_size("ta"))]],
    )
    places = [near_groups[0].index(member) for member in gather_groups[0]]
    correlator = pl.pallas_call(
        functools.partial(scale_kernel, places, all_sites),
        out_shape=jax.ShapeDtypeStruct((near * rows, lanes), jnp.float32),
        in_specs=[IN_VMEM] * 2,
        out_specs=IN_HBM,
        scratch_shapes=[
            pltpu.VMEM((near * rows, lanes), jnp.float32),
            pltpu.SemaphoreType.DMA((4,)),
        ],
        compiler_params=SMALL,
    )(gathered, picked)
    return correlator.reshape(pairs, slices, lanes)


def solution(mesh):
    near_groups, far_groups, gather_groups = groups(mesh.shape["xy"], mesh.shape["gz"])
    return jax.shard_map(
        functools.partial(on_device, near_groups, far_groups, gather_groups),
        mesh=mesh,
        in_specs=(P(None, None, None, None, "ta", SITE_AXES), P(None, SITE_AXES), P(), P()),
        out_specs=P(None, "ta", None),
        check_vma=False,
    )
```
